32 devices in a mesh: tm: 8 (over z, x), pair: 4 (over y, core).
Axes of the slice: x: 2, y: 2, z: 4, core: 2. Of those that a mesh axis runs over, the one named last changes fastest.
Arguments:
- signal: float32 [2, 131072], P(None, 'tm'), may hold values from -6 to 6
- hop_offsets: int32 [2048], P(('tm', 'pair')), may hold values from 0 to 131071, as said below
- pair_channels: int32 [2, 8192], P(None, 'pair'), may hold values from 0 to 255
Outputs:
- surface: float32 [64, 8192], P(None, 'pair')
The draws below stay inside these ranges and needn't reach their ends.
Inputs may be any that keep to these rules, and one draw needn't show every extreme that they name: `hop_offsets`: hop p starts at a sample in p * 64 to p * 64 + 63.
All inputs are finite; a program needn't handle non-finite values.
Results may differ from the reference program's by a relative error of at most 0.000071.
Values sent between devices are 32-bit elements; how exact they have to be, the bound alone decides.
A program may use at most 64 MiB of HBM per device.

```python
import math
import jax
import jax.numpy as jnp
from jax import lax

NP = 256
Q = 64
STRIDE = 64
HOPS = 2048
SAMPLES = 131072
PAIRS = 8192
NBLK = 32


def draw_hop_offsets(key, part):
    jitter = jax.random.randint(jax.random.fold_in(key, 11), (HOPS,), 0, STRIDE, dtype=jnp.int32)
    return jnp.arange(HOPS, dtype=jnp.int32) * STRIDE + jitter


def with_ends(values, stream_key, smallest, largest):
    shape = values.shape
    spot = [jax.random.randint(jax.random.fold_in(stream_key, axis), (), 0, shape[axis]) for axis in range(len(shape))]
    values = values.at[tuple(spot)].set(smallest)
    longest = shape.index(max(shape))
    spot[longest] = (spot[longest] + 1) % shape[longest]
    return values.at[tuple(spot)].set(largest)


def level_of(rng, dims, pieces, least, high):
    factor_of = 1.0
    for dim, blocks in pieces:
        draws = jax.random.uniform(jax.random.fold_in(jax.random.fold_in(rng, 6), dim), (blocks,), jnp.float32, least / len(pieces), high / len(pieces))
        factor_of = factor_of * jnp.repeat(jnp.exp(draws), dims[dim] // blocks).reshape((-1,) + (1,) * (len(dims) - 1 - dim))
    return factor_of


def centred(key, shape, deviation, most, split=(), held_as=jnp.bfloat16):
    array = deviation * jax.random.normal(key, shape, jnp.float32)
    if split:
        array = array * level_of(key, shape, split, -0.22, 0.18)
    return jnp.clip(array, -most, most).astype(held_as)


def setup_inputs(seed: int = 0) -> dict:
    splits = jax.random.split(jax.random.key(seed), 4)
    return {
        "signal": centred(splits[0], (2, SAMPLES), 1.0, 6.0, ((1, 8),), jnp.float32),
        "hop_offsets": draw_hop_offsets(jax.random.fold_in(splits[3], 71), 0),
        "pair_channels": with_ends(jax.random.randint(splits[2], (2, PAIRS), 0, NP), jax.random.fold_in(splits[2], 1), 0, NP - 1).astype(jnp.int32),
    }


def reference(signal, hop_offsets, pair_channels):
    extended = jnp.concatenate([signal, jnp.zeros((2, NP), signal.dtype)], axis=1)
    sample = jnp.arange(NP, dtype=jnp.int32)
    window = 0.54 - 0.46 * jnp.cos(2.0 * jnp.pi * sample.astype(signal.dtype) / NP)
    gainval = 1.0 / jnp.sqrt(jnp.sum(window * window))
    spots = hop_offsets[:, None] + sample[None, :]
    frames = (extended[0][spots] + 1j * extended[1][spots]) * window[None, :]
    spectra = jnp.fft.fft(frames, axis=1) * gainval
    turns = sample[None, :] * (hop_offsets[:, None] % NP) % NP
    theta = 2.0 * jnp.pi * turns.astype(signal.dtype) / NP
    spectra = spectra * jnp.exp(-1j * theta)
    width = math.gcd(PAIRS, 1024)
    grouped = pair_channels.reshape(2, PAIRS // width, width).transpose(1, 0, 2)

    def block_power(index):
        first = spectra[:, index[0]]
        second = spectra[:, index[1]]
        products = (first * jnp.conj(second)).reshape(NBLK, Q, width)
        cyclic = jnp.fft.fft(products, axis=1) / math.sqrt(Q)
        return lax.optimization_barrier(jnp.sum(jnp.real(cyclic) ** 2 + jnp.imag(cyclic) ** 2, axis=0))
    powers = lax.map(block_power, grouped)
    return powers.transpose(1, 0, 2).reshape(Q, PAIRS) / NBLK
```

```python
import functools
import math

import jax
import jax.numpy as jnp
import numpy as np
from jax import lax
from jax.experimental import pallas as pl
from jax.experimental.pallas import tpu as pltpu
from jax.sharding import PartitionSpec as P

NP = 256
Q = 64
STRIDE = 64
SLOTS = NP // STRIDE
GROUP = Q // SLOTS
MESH = pl.DeviceIdType.MESH


def split_table(table):
    high = table.astype(jnp.bfloat16)
    low = (table - high.astype(np.float64)).astype(jnp.bfloat16)
    return high, low


def first_table():
    sample = np.arange(NP)
    angle = 2.0 * np.pi * (sample[:, None] * sample[None, :] % NP) / NP
    window = 0.54 - 0.46 * np.cos(2.0 * np.pi * sample / NP)
    gainval = 1.0 / np.sqrt(np.sum(window * window))
    return np.concatenate([np.cos(angle), np.sin(angle)], axis=0) * gainval


def hop_order():
    place = np.arange(Q)
    return place % GROUP * SLOTS + place // GROUP


def second_table():
    angle = 2.0 * np.pi * (np.arange(Q)[:, None] * hop_order()[None, :] % Q) / Q
    cosine = np.cos(angle) / math.sqrt(Q)
    sine = np.sin(angle) / math.sqrt(Q)
    upper = np.concatenate([cosine, sine], axis=1)
    lower = np.concatenate([-sine, cosine], axis=1)
    return np.concatenate([upper, lower], axis=0)


def parts_of(value):
    high = value.astype(jnp.bfloat16)
    return high, (value - high.astype(jnp.float32)).astype(jnp.bfloat16)


def dot(left, right):
    return jnp.dot(left, right, preferred_element_type=jnp.float32)


def kernel(
    devices, groups, chunks, width, total_blocks,
    signal, offsets, index, first_high, first_low, second_both, second_low,
    out,
    all_offsets, halo, spectra, partial, received, finished,
    offset_send, offset_recv, halo_send, halo_recv, part_send, part_recv, done_send, done_recv,
):
    me = lax.axis_index("tm")
    mine = lax.axis_index("pair")
    rows = signal.shape[1]
    blocks = rows // GROUP

    barrier = pltpu.get_barrier_semaphore()
    for step in range(1, devices):
        pl.semaphore_signal(barrier, inc=1, device_id={"tm": lax.rem(me + step, devices)}, device_id_type=MESH)
    for step in range(1, groups):
        pl.semaphore_signal(barrier, inc=1, device_id={"pair": lax.rem(mine + step, groups)}, device_id_type=MESH)
    pl.semaphore_wait(barrier, devices + groups - 2)

    edge = pltpu.make_async_remote_copy(
        src_ref=signal.at[:, 0:8, :], dst_ref=halo, send_sem=halo_send, recv_sem=halo_recv,
        device_id={"tm": lax.rem(me + devices - 1, devices)}, device_id_type=MESH,
    )
    edge.start()
    moves = []
    for step in range(1, groups):
        move = pltpu.make_async_remote_copy(
            src_ref=offsets, dst_ref=all_offsets.at[mine],
            send_sem=offset_send.at[step], recv_sem=offset_recv.at[step],
            device_id={"pair": lax.rem(mine + step, groups)}, device_id_type=MESH,
        )
        move.start()
        moves.append(move)
    all_offsets[mine] = offsets[...]
    for move in moves:
        move.wait()
    edge.wait()

    place = jnp.bitwise_and(all_offsets[...].reshape(rows, SLOTS), NP - 1)
    turn = place.astype(jnp.float32) * (2.0 * math.pi / NP)
    cosines = jnp.cos(turn) * 0.46
    sines = jnp.sin(turn) * 0.46
    sample = lax.broadcasted_iota(jnp.int32, (rows, NP), 1)
    around = lax.broadcasted_iota(jnp.int32, (1, NP), 1).astype(jnp.float32) * (2.0 * math.pi / NP)
    cosine_row = jnp.cos(around)
    sine_row = jnp.sin(around)
    keep = jnp.where(me == devices - 1, 0.0, 1.0)
    real = signal[0]
    imag = signal[1]
    real_next = jnp.concatenate([real[1:], halo[0, 0:1] * keep], axis=0)
    imag_next = jnp.concatenate([imag[1:], halo[1, 0:1] * keep], axis=0)
    for slot in range(SLOTS):
        where = place[:, slot : slot + 1]
        weight = 0.54 - (cosines[:, slot : slot + 1] * cosine_row + sines[:, slot : slot + 1] * sine_row)
        later = sample < where
        frame_re = jnp.where(later, real_next, real) * weight
        frame_im = jnp.where(later, imag_next, imag) * weight
        upper = jnp.concatenate([frame_re, frame_im], axis=1)
        lower = jnp.concatenate([frame_im, -frame_re], axis=1)
        high, low = parts_of(jnp.concatenate([upper, lower], axis=0))
        result = dot(high, first_high[...]) + dot(low, first_high[...]) + dot(high, first_low[...])
        high, low = parts_of(result)
        both = jnp.concatenate([high, low], axis=1)
        for block in range(blocks):
            at = block * Q + slot * GROUP
            for half in range(2):
                spectra[half * blocks * Q + at : half * blocks * Q + at + GROUP, :] = both[
                    half * rows + block * GROUP : half * rows + (block + 1) * GROUP
                ]

    channel = jnp.bitwise_and(lax.broadcasted_iota(jnp.int32, (2 * NP, width), 0), NP - 1)
    half_rows = blocks * Q
    part_moves = []
    done_moves = []

    def compute(chunk):
        columns = slice(chunk * width, (chunk + 1) * width)
        pick_first = jnp.where(channel == index[0:1, columns], 1.0, 0.0).astype(jnp.bfloat16)
        pick_second = jnp.where(channel == index[1:2, columns], 1.0, 0.0).astype(jnp.bfloat16)
        power = jnp.zeros((Q, width), jnp.float32)
        for block in range(blocks):
            re_rows = slice(block * Q, (block + 1) * Q)
            im_rows = slice(half_rows + block * Q, half_rows + (block + 1) * Q)
            wave = jnp.concatenate([spectra[re_rows, :], spectra[im_rows, :]], axis=0)
            first = dot(wave, pick_first)
            second = dot(wave, pick_second)
            product_re = first[:Q] * second[:Q] + first[Q:] * second[Q:]
            product_im = first[Q:] * second[:Q] - first[:Q] * second[Q:]
            high, low = parts_of(jnp.concatenate([product_re, product_im], axis=0))
            cyclic = dot(second_both[...], jnp.concatenate([high, low], axis=0)) + dot(second_low[...], high)
            squared = cyclic * cyclic
            power = power + (squared[:Q] + squared[Q:])
        share = Q // devices
        for device in range(devices):
            partial[chunk, device] = power[device * share : (device + 1) * share]
        for step in range(1, devices):
            to = lax.rem(me + step, devices)
            move = pltpu.make_async_remote_copy(
                src_ref=partial.at[chunk, to], dst_ref=received.at[chunk, step],
                send_sem=part_send.at[chunk, step], recv_sem=part_recv.at[chunk, step],
                device_id={"tm": to}, device_id_type=MESH,
            )
            move.start()
            part_moves.append((chunk, move))

    def reduce(chunk):
        columns = slice(chunk * width, (chunk + 1) * width)
        total = partial[chunk, me]
        for which, move in part_moves:
            if which == chunk:
                move.wait_recv()
        for step in range(1, devices):
            total = total + received[chunk, step]
        total = total * (1.0 / total_blocks)
        finished[chunk] = total
        out[me, :, columns] = total
        for step in range(1, devices):
            move = pltpu.make_async_remote_copy(
                src_ref=finished.at[chunk], dst_ref=out.at[me, :, columns],
                send_sem=done_send.at[chunk, step], recv_sem=done_recv.at[chunk, step],
                device_id={"tm": lax.rem(me + step, devices)}, device_id_type=MESH,
            )
            move.start()
            done_moves.append(move)

    for chunk in range(chunks):
        compute(chunk)
        if chunk >= 2:
            reduce(chunk - 2)
    for chunk in range(max(chunks - 2, 0), chunks):
        reduce(chunk)
    for which, move in part_moves:
        move.wait_send()
    for move in done_moves:
        move.wait()


def shards(devices, groups, signal, hop_offsets, pair_channels):
    span = signal.shape[1]
    rows = span // NP
    local_pairs = pair_channels.shape[1]
    width = math.gcd(local_pairs, 512)
    chunks = local_pairs // width
    share = Q // devices
    own_rows = hop_offsets.shape[0] // SLOTS
    blocks = rows // GROUP
    first_high, first_low = split_table(first_table())
    second_high, second_low = split_table(second_table())
    second_both = np.concatenate([second_high, second_high], axis=1)
    vmem = pl.BlockSpec(memory_space=pltpu.VMEM)
    dma = pltpu.SemaphoreType.DMA
    surface = pl.pallas_call(
        functools.partial(kernel, devices, groups, chunks, width, blocks * devices),
        out_shape=jax.ShapeDtypeStruct((devices, share, local_pairs), jnp.float32),
        in_specs=[vmem] * 7,
        out_specs=vmem,
        scratch_shapes=[
            pltpu.VMEM((groups, own_rows, SLOTS), jnp.int32),
            pltpu.VMEM((2, 8, NP), jnp.float32),
            pltpu.VMEM((2 * blocks * Q, 2 * NP), jnp.bfloat16),
            pltpu.VMEM((chunks, devices, share, width), jnp.float32),
            pltpu.VMEM((chunks, devices, share, width), jnp.float32),
            pltpu.VMEM((chunks, share, width), jnp.float32),
            dma((groups,)), dma((groups,)), dma, dma,
            dma((chunks, devices)), dma((chunks, devices)), dma((chunks, devices)), dma((chunks, devices)),
        ],
        compiler_params=pltpu.CompilerParams(collective_id=0, has_side_effects=True),
    )(
        signal.reshape(2, rows, NP), hop_offsets.reshape(own_rows, SLOTS), pair_channels,
        first_high, first_low, second_both, second_low,
    )
    return surface.reshape(Q, local_pairs)


def solution(mesh):
    return jax.shard_map(
        functools.partial(shards, mesh.shape["tm"], mesh.shape["pair"]),
        mesh=mesh,
        in_specs=(P(None, "tm"), P(("tm", "pair")), P(None, "pair")),
        out_specs=P(None, "pair"),
        check_vma=False,
    )
```

```python
import functools
import math

import jax
import jax.numpy as jnp
import numpy as np
from jax import lax
from jax.experimental import pallas as pl
from jax.experimental.pallas import tpu as pltpu
from jax.sharding import PartitionSpec as P

NP = 256
Q = 64
STRIDE = 64
SLOTS = NP // STRIDE
GROUP = Q // SLOTS
MESH = pl.DeviceIdType.MESH


def split_table(table):
    high = table.astype(jnp.bfloat16)
    low = (table - high.astype(np.float64)).astype(jnp.bfloat16)
    return high, low


def first_table():
    sample = np.arange(NP)
    angle = 2.0 * np.pi * (sample[:, None] * sample[None, :] % NP) / NP
    window = 0.54 - 0.46 * np.cos(2.0 * np.pi * sample / NP)
    gainval = 1.0 / np.sqrt(np.sum(window * window))
    return np.concatenate([np.cos(angle), np.sin(angle)], axis=0) * gainval


def hop_order():
    place = np.arange(Q)
    return place % GROUP * SLOTS + place // GROUP


def second_table():
    angle = 2.0 * np.pi * (np.arange(Q)[:, None] * hop_order()[None, :] % Q) / Q
    cosine = np.cos(angle) / math.sqrt(Q)
    sine = np.sin(angle) / math.sqrt(Q)
    upper = np.concatenate([cosine, sine], axis=1)
    lower = np.concatenate([-sine, cosine], axis=1)
    return np.concatenate([upper, lower], axis=0)


def parts_of(value):
    high = value.astype(jnp.bfloat16)
    return high, (value - high.astype(jnp.float32)).astype(jnp.bfloat16)


def dot(left, right):
    return jnp.dot(left, right, preferred_element_type=jnp.float32)


def kernel(
    inner, outer, groups, chunks, width, total_blocks,
    signal, offsets, index, first_high, first_low, second_both, second_low,
    out,
    all_offsets, halo, spectra, partial, near, joined, far, finished,
    offset_send, offset_recv, halo_send, halo_recv,
    near_send, near_recv, far_send, far_recv, back_send, back_recv, done_send, done_recv,
):
    me = lax.axis_index("tm")
    mine = lax.axis_index("pair")
    devices = inner * outer
    across = lax.rem(me, inner)
    along = me // inner
    rows = signal.shape[1]
    blocks = rows // GROUP

    def near_peer(step):
        place = lax.rem(across + step, inner)
        return place, {"tm": along * inner + place}

    def far_peer(step):
        place = lax.rem(along + step, outer)
        return place, {"tm": place * inner + across}

    barrier = pltpu.get_barrier_semaphore()

    def greet(device):
        pl.semaphore_signal(barrier, inc=1, device_id=device, device_id_type=MESH)

    for step in range(1, inner):
        greet(near_peer(step)[1])
    for step in range(1, outer):
        greet(far_peer(step)[1])
    for step in range(1, groups):
        greet({"pair": lax.rem(mine + step, groups)})

    @pl.when(me > 0)
    def _():
        greet({"tm": me - 1})

    @pl.when(me < devices - 1)
    def _():
        greet({"tm": me + 1})

    ends = jnp.where(me > 0, 1, 0) + jnp.where(me < devices - 1, 1, 0)
    pl.semaphore_wait(barrier, inner + outer + groups - 3 + ends)

    edge = pltpu.make_async_remote_copy(
        src_ref=signal.at[:, 0:8, :], dst_ref=halo, send_sem=halo_send, recv_sem=halo_recv,
        device_id={"tm": lax.rem(me + devices - 1, devices)}, device_id_type=MESH,
    )

    @pl.when(me > 0)
    def _():
        edge.start()

    @pl.when(me == devices - 1)
    def _():
        halo[...] = jnp.zeros_like(halo)

    hellos = []
    for step in range(1, groups):
        move = pltpu.make_async_remote_copy(
            src_ref=offsets, dst_ref=all_offsets.at[mine],
            send_sem=offset_send.at[step], recv_sem=offset_recv.at[step],
            device_id={"pair": lax.rem(mine + step, groups)}, device_id_type=MESH,
        )
        move.start()
        hellos.append(move)
    all_offsets[mine] = offsets[...]
    for move in hellos:
        move.wait()

    @pl.when(me > 0)
    def _():
        edge.wait_send()

    @pl.when(me < devices - 1)
    def _():
        edge.wait_recv()

    place = jnp.bitwise_and(all_offsets[...].reshape(rows, SLOTS), NP - 1)
    turn = place.astype(jnp.float32) * (2.0 * math.pi / NP)
    cosines = jnp.cos(turn) * 0.46
    sines = jnp.sin(turn) * 0.46
    sample = lax.broadcasted_iota(jnp.int32, (rows, NP), 1)
    around = lax.broadcasted_iota(jnp.int32, (1, NP), 1).astype(jnp.float32) * (2.0 * math.pi / NP)
    cosine_row = jnp.cos(around)
    sine_row = jnp.sin(around)
    real = signal[0]
    imag = signal[1]
    real_next = jnp.concatenate([real[1:], halo[0, 0:1]], axis=0)
    imag_next = jnp.concatenate([imag[1:], halo[1, 0:1]], axis=0)
    for slot in range(SLOTS):
        where = place[:, slot : slot + 1]
        weight = 0.54 - (cosines[:, slot : slot + 1] * cosine_row + sines[:, slot : slot + 1] * sine_row)
        later = sample < where
        frame_re = jnp.where(later, real_next, real) * weight
        frame_im = jnp.where(later, imag_next, imag) * weight
        upper = jnp.concatenate([frame_re, frame_im], axis=1)
        lower = jnp.concatenate([frame_im, -frame_re], axis=1)
        high, low = parts_of(jnp.concatenate([upper, lower], axis=0))
        result = dot(high, first_high[...]) + dot(low, first_high[...]) + dot(high, first_low[...])
        high, low = parts_of(result)
        both = jnp.concatenate([high, low], axis=1)
        for block in range(blocks):
            at = block * Q + slot * GROUP
            for half in range(2):
                spectra[half * blocks * Q + at : half * blocks * Q + at + GROUP, :] = both[
                    half * rows + block * GROUP : half * rows + (block + 1) * GROUP
                ]

    channel = jnp.bitwise_and(lax.broadcasted_iota(jnp.int32, (2 * NP, width), 0), NP - 1)
    half_rows = blocks * Q
    share = Q // devices
    moves = {}

    def send(name, chunk, step, source, target, sems, device):
        move = pltpu.make_async_remote_copy(
            src_ref=source, dst_ref=target, send_sem=sems[0].at[chunk, step], recv_sem=sems[1].at[chunk, step],
            device_id=device, device_id_type=MESH,
        )
        move.start()
        moves.setdefault((name, chunk), []).append(move)

    def arrive(name, chunk):
        for move in moves.get((name, chunk), []):
            move.wait_recv()

    def compute(chunk):
        columns = slice(chunk * width, (chunk + 1) * width)
        pick_first = jnp.where(channel == index[0:1, columns], 1.0, 0.0).astype(jnp.bfloat16)
        pick_second = jnp.where(channel == index[1:2, columns], 1.0, 0.0).astype(jnp.bfloat16)
        power = jnp.zeros((Q, width), jnp.float32)
        for block in range(blocks):
            re_rows = slice(block * Q, (block + 1) * Q)
            im_rows = slice(half_rows + block * Q, half_rows + (block + 1) * Q)
            wave = jnp.concatenate([spectra[re_rows, :], spectra[im_rows, :]], axis=0)
            first = dot(wave, pick_first)
            second = dot(wave, pick_second)
            product_re = first[:Q] * second[:Q] + first[Q:] * second[Q:]
            product_im = first[Q:] * second[:Q] - first[:Q] * second[Q:]
            high, low = parts_of(jnp.concatenate([product_re, product_im], axis=0))
            cyclic = dot(second_both[...], jnp.concatenate([high, low], axis=0)) + dot(second_low[...], high)
            squared = cyclic * cyclic
            power = power + (squared[:Q] + squared[Q:])
        for place in range(inner):
            for other in range(outer):
                at = (place * outer + other) * share
                partial[chunk, place, other] = power[at : at + share]
        for step in range(1, inner):
            place, device = near_peer(step)
            send("near", chunk, step, partial.at[chunk, place], near.at[chunk, step], (near_send, near_recv), device)

    def join(chunk):
        total = partial[chunk, across]
        arrive("near", chunk)
        for step in range(1, inner):
            total = total + near[chunk, step]
        joined[chunk] = total
        for step in range(1, outer):
            place, device = far_peer(step)
            send("far", chunk, step, joined.at[chunk, place], far.at[chunk, step], (far_send, far_recv), device)

    def finish(chunk):
        columns = slice(chunk * width, (chunk + 1) * width)
        total = joined[chunk, along]
        arrive("far", chunk)
        for step in range(1, outer):
            total = total + far[chunk, step]
        total = total * (1.0 / total_blocks)
        finished[chunk] = total
        out[across, along, :, columns] = total
        for step in range(1, outer):
            target = out.at[across, along, :, columns]
            send("back", chunk, step, finished.at[chunk], target, (back_send, back_recv), far_peer(step)[1])

    def spread(chunk):
        columns = slice(chunk * width, (chunk + 1) * width)
        arrive("back", chunk)
        for step in range(1, inner):
            line = out.at[across, :, :, columns]
            send("done", chunk, step, line, line, (done_send, done_recv), near_peer(step)[1])

    stages = ((compute, 0), (join, 3), (finish, 6), (spread, 9))
    for tick in range(chunks + stages[-1][1]):
        for stage, lag in stages:
            if 0 <= tick - lag < chunks:
                stage(tick - lag)
    for chunk in range(chunks):
        arrive("done", chunk)
    for group in moves.values():
        for move in group:
            move.wait_send()


def shards(devices, groups, signal, hop_offsets, pair_channels):
    span = signal.shape[1]
    rows = span // NP
    local_pairs = pair_channels.shape[1]
    width = math.gcd(local_pairs, 256)
    chunks = local_pairs // width
    inner = 1 << (devices.bit_length() - 1) // 2
    outer = devices // inner
    share = Q // devices
    own_rows = hop_offsets.shape[0] // SLOTS
    blocks = rows // GROUP
    first_high, first_low = split_table(first_table())
    second_high, second_low = split_table(second_table())
    second_both = np.concatenate([second_high, second_high], axis=1)
    vmem = pl.BlockSpec(memory_space=pltpu.VMEM)
    dma = pltpu.SemaphoreType.DMA
    surface = pl.pallas_call(
        functools.partial(kernel, inner, outer, groups, chunks, width, blocks * devices),
        out_shape=jax.ShapeDtypeStruct((inner, outer, share, local_pairs), jnp.float32),
        in_specs=[vmem] * 7,
        out_specs=vmem,
        scratch_shapes=[
            pltpu.VMEM((groups, own_rows, SLOTS), jnp.int32),
            pltpu.VMEM((2, 8, NP), jnp.float32),
            pltpu.VMEM((2 * blocks * Q, 2 * NP), jnp.bfloat16),
            pltpu.VMEM((chunks, inner, outer, share, width), jnp.float32),
            pltpu.VMEM((chunks, inner, outer, share, width), jnp.float32),
            pltpu.VMEM((chunks, outer, share, width), jnp.float32),
            pltpu.VMEM((chunks, outer, share, width), jnp.float32),
            pltpu.VMEM((chunks, share, width), jnp.float32),
            dma((groups,)), dma((groups,)), dma, dma,
            dma((chunks, inner)), dma((chunks, inner)), dma((chunks, outer)), dma((chunks, outer)),
            dma((chunks, outer)), dma((chunks, outer)), dma((chunks, inner)), dma((chunks, inner)),
        ],
        compiler_params=pltpu.CompilerParams(collective_id=0, has_side_effects=True),
    )(
        signal.reshape(2, rows, NP), hop_offsets.reshape(own_rows, SLOTS), pair_channels,
        first_high, first_low, second_both, second_low,
    )
    return surface.reshape(Q, local_pairs)


def solution(mesh):
    return jax.shard_map(
        functools.partial(shards, mesh.shape["tm"], mesh.shape["pair"]),
        mesh=mesh,
        in_specs=(P(None, "tm"), P(("tm", "pair")), P(None, "pair")),
        out_specs=P(None, "pair"),
        check_vma=False,
    )
```

```python
import functools
import math

import jax
import jax.numpy as jnp
import numpy as np
from jax import lax
from jax.experimental import pallas as pl
from jax.experimental.pallas import tpu as pltpu
from jax.sharding import PartitionSpec as P

NP = 256
Q = 64
STRIDE = 64
SLOTS = NP // STRIDE
GROUP = Q // SLOTS
MESH = pl.DeviceIdType.MESH


def split_table(table):
    high = table.astype(jnp.bfloat16)
    low = (table - high.astype(np.float64)).astype(jnp.bfloat16)
    return high, low


def first_table():
    sample = np.arange(NP)
    angle = 2.0 * np.pi * (sample[:, None] * sample[None, :] % NP) / NP
    window = 0.54 - 0.46 * np.cos(2.0 * np.pi * sample / NP)
    gainval = 1.0 / np.sqrt(np.sum(window * window))
    return np.concatenate([np.cos(angle), np.sin(angle)], axis=0) * gainval


def hop_order():
    place = np.arange(Q)
    return place % GROUP * SLOTS + place // GROUP


def second_table():
    angle = 2.0 * np.pi * (np.arange(Q)[:, None] * hop_order()[None, :] % Q) / Q
    cosine = np.cos(angle) / math.sqrt(Q)
    sine = np.sin(angle) / math.sqrt(Q)
    upper = np.concatenate([cosine, sine], axis=1)
    lower = np.concatenate([-sine, cosine], axis=1)
    return np.concatenate([upper, lower], axis=0)


def parts_of(value):
    high = value.astype(jnp.bfloat16)
    return high, (value - high.astype(jnp.float32)).astype(jnp.bfloat16)


def dot(left, right):
    return jnp.dot(left, right, preferred_element_type=jnp.float32)


def kernel(
    inner, outer, groups, chunks, width, total_blocks,
    signal, offsets, index, first_high, first_low, second_both, second_low,
    out,
    samples, all_offsets, halo, spectra, partial, near, joined, far, finished,
    offset_send, offset_recv, halo_send, halo_recv,
    near_send, near_recv, far_send, far_recv, back_send, back_recv, done_send, done_recv,
):
    me = lax.axis_index("tm")
    mine = lax.axis_index("pair")
    devices = inner * outer
    across = lax.rem(me, inner)
    along = me // inner
    rows = samples.shape[1]
    blocks = rows // GROUP

    def near_peer(step):
        place = lax.rem(across + step, inner)
        return place, {"tm": along * inner + place}

    def far_peer(step):
        place = lax.rem(along + step, outer)
        return place, {"tm": place * inner + across}

    barrier = pltpu.get_barrier_semaphore()

    def greet(device):
        pl.semaphore_signal(barrier, inc=1, device_id=device, device_id_type=MESH)

    for step in range(1, inner):
        greet(near_peer(step)[1])
    for step in range(1, outer):
        greet(far_peer(step)[1])
    for step in range(1, groups):
        greet({"pair": lax.rem(mine + step, groups)})

    @pl.when(me > 0)
    def _():
        greet({"tm": me - 1})

    @pl.when(me < devices - 1)
    def _():
        greet({"tm": me + 1})

    for row in range(rows):
        samples[:, row, :] = signal[:, row * NP : (row + 1) * NP]

    ends = jnp.where(me > 0, 1, 0) + jnp.where(me < devices - 1, 1, 0)
    pl.semaphore_wait(barrier, inner + outer + groups - 3 + ends)

    edge = pltpu.make_async_remote_copy(
        src_ref=signal.at[:, 0:NP], dst_ref=halo, send_sem=halo_send, recv_sem=halo_recv,
        device_id={"tm": lax.rem(me + devices - 1, devices)}, device_id_type=MESH,
    )

    @pl.when(me > 0)
    def _():
        edge.start()

    @pl.when(me == devices - 1)
    def _():
        halo[...] = jnp.zeros_like(halo)

    hellos = []
    for step in range(1, groups):
        move = pltpu.make_async_remote_copy(
            src_ref=offsets, dst_ref=all_offsets.at[mine],
            send_sem=offset_send.at[step], recv_sem=offset_recv.at[step],
            device_id={"pair": lax.rem(mine + step, groups)}, device_id_type=MESH,
        )
        move.start()
        hellos.append(move)
    all_offsets[mine] = offsets[...]
    for move in hellos:
        move.wait()

    @pl.when(me > 0)
    def _():
        edge.wait_send()

    @pl.when(me < devices - 1)
    def _():
        edge.wait_recv()

    own_hops = offsets.shape[1]
    own_rows = own_hops // SLOTS
    hop = lax.broadcasted_iota(jnp.int32, (own_rows, own_hops), 1)
    first_hop = lax.broadcasted_iota(jnp.int32, (own_rows, own_hops), 0) * SLOTS
    lane = lax.broadcasted_iota(jnp.int32, (own_rows, SLOTS), 1)
    places = []
    for group in range(groups):
        line = jnp.bitwise_and(all_offsets[group], NP - 1).astype(jnp.float32)
        place = jnp.zeros((own_rows, SLOTS), jnp.float32)
        for slot in range(SLOTS):
            chosen = jnp.where(hop == first_hop + slot, line, 0.0)
            place = jnp.where(lane == slot, jnp.sum(chosen, axis=1, keepdims=True), place)
        places.append(place)
    place = jnp.concatenate(places, axis=0)
    turn = place * (2.0 * math.pi / NP)
    place = place.astype(jnp.int32)
    cosines = jnp.cos(turn) * 0.46
    sines = jnp.sin(turn) * 0.46
    sample = lax.broadcasted_iota(jnp.int32, (rows, NP), 1)
    around = lax.broadcasted_iota(jnp.int32, (1, NP), 1).astype(jnp.float32) * (2.0 * math.pi / NP)
    cosine_row = jnp.cos(around)
    sine_row = jnp.sin(around)
    real = samples[0]
    imag = samples[1]
    real_next = jnp.concatenate([real[1:], halo[0:1]], axis=0)
    imag_next = jnp.concatenate([imag[1:], halo[1:2]], axis=0)
    for slot in range(SLOTS):
        where = place[:, slot : slot + 1]
        weight = 0.54 - (cosines[:, slot : slot + 1] * cosine_row + sines[:, slot : slot + 1] * sine_row)
        later = sample < where
        frame_re = jnp.where(later, real_next, real) * weight
        frame_im = jnp.where(later, imag_next, imag) * weight
        upper = jnp.concatenate([frame_re, frame_im], axis=1)
        lower = jnp.concatenate([frame_im, -frame_re], axis=1)
        high, low = parts_of(jnp.concatenate([upper, lower], axis=0))
        result = dot(high, first_high[...]) + dot(low, first_high[...]) + dot(high, first_low[...])
        high, low = parts_of(result)
        both = jnp.concatenate([high, low], axis=1)
        for block in range(blocks):
            at = block * Q + slot * GROUP
            for half in range(2):
                spectra[half * blocks * Q + at : half * blocks * Q + at + GROUP, :] = both[
                    half * rows + block * GROUP : half * rows + (block + 1) * GROUP
                ]

    channel = jnp.bitwise_and(lax.broadcasted_iota(jnp.int32, (2 * NP, width), 0), NP - 1)
    half_rows = blocks * Q
    share = Q // devices
    moves = {}

    def send(name, chunk, step, source, target, sems, device):
        move = pltpu.make_async_remote_copy(
            src_ref=source, dst_ref=target, send_sem=sems[0].at[chunk, step], recv_sem=sems[1].at[chunk, step],
            device_id=device, device_id_type=MESH,
        )
        move.start()
        moves.setdefault((name, chunk), []).append(move)

    def arrive(name, chunk):
        for move in moves.get((name, chunk), []):
            move.wait_recv()

    def compute(chunk):
        columns = slice(chunk * width, (chunk + 1) * width)
        pick_first = jnp.where(channel == index[0:1, columns], 1.0, 0.0).astype(jnp.bfloat16)
        pick_second = jnp.where(channel == index[1:2, columns], 1.0, 0.0).astype(jnp.bfloat16)
        power = jnp.zeros((Q, width), jnp.float32)
        for block in range(blocks):
            re_rows = slice(block * Q, (block + 1) * Q)
            im_rows = slice(half_rows + block * Q, half_rows + (block + 1) * Q)
            wave = jnp.concatenate([spectra[re_rows, :], spectra[im_rows, :]], axis=0)
            first = dot(wave, pick_first)
            second = dot(wave, pick_second)
            product_re = first[:Q] * second[:Q] + first[Q:] * second[Q:]
            product_im = first[Q:] * second[:Q] - first[:Q] * second[Q:]
            high, low = parts_of(jnp.concatenate([product_re, product_im], axis=0))
            cyclic = dot(second_both[...], jnp.concatenate([high, low], axis=0)) + dot(second_low[...], high)
            squared = cyclic * cyclic
            power = power + (squared[:Q] + squared[Q:])
        for place in range(inner):
            for other in range(outer):
                at = (place * outer + other) * share
                partial[chunk, place, other] = power[at : at + share]
        for step in range(1, inner):
            place, device = near_peer(step)
            send("near", chunk, step, partial.at[chunk, place], near.at[chunk, step], (near_send, near_recv), device)

    def join(chunk):
        total = partial[chunk, across]
        arrive("near", chunk)
        for step in range(1, inner):
            total = total + near[chunk, step]
        joined[chunk] = total
        for step in range(1, outer):
            place, device = far_peer(step)
            send("far", chunk, step, joined.at[chunk, place], far.at[chunk, step], (far_send, far_recv), device)

    def finish(chunk):
        columns = slice(chunk * width, (chunk + 1) * width)
        total = joined[chunk, along]
        arrive("far", chunk)
        for step in range(1, outer):
            total = total + far[chunk, step]
        total = total * (1.0 / total_blocks)
        finished[chunk] = total
        out[across, along, :, columns] = total
        for step in range(1, outer):
            target = out.at[across, along, :, columns]
            send("back", chunk, step, finished.at[chunk], target, (back_send, back_recv), far_peer(step)[1])

    def spread(chunk):
        columns = slice(chunk * width, (chunk + 1) * width)
        arrive("back", chunk)
        for step in range(1, inner):
            line = out.at[across, :, :, columns]
            send("done", chunk, step, line, line, (done_send, done_recv), near_peer(step)[1])

    stages = ((compute, 0), (join, 1), (finish, 2), (spread, 3))
    for tick in range(chunks + stages[-1][1]):
        for stage, lag in stages:
            if 0 <= tick - lag < chunks:
                stage(tick - lag)
    for chunk in range(chunks):
        arrive("done", chunk)
    for group in moves.values():
        for move in group:
            move.wait_send()


def shards(devices, groups, signal, hop_offsets, pair_channels):
    span = signal.shape[1]
    rows = span // NP
    local_pairs = pair_channels.shape[1]
    width = math.gcd(local_pairs, 512)
    chunks = local_pairs // width
    inner = 1 << (devices.bit_length() - 1) // 2
    outer = devices // inner
    share = Q // devices
    own_rows = hop_offsets.shape[0] // SLOTS
    blocks = rows // GROUP
    first_high, first_low = split_table(first_table())
    second_high, second_low = split_table(second_table())
    second_both = np.concatenate([second_high, second_high], axis=1)
    vmem = pl.BlockSpec(memory_space=pltpu.VMEM)
    dma = pltpu.SemaphoreType.DMA
    surface = pl.pallas_call(
        functools.partial(kernel, inner, outer, groups, chunks, width, blocks * devices),
        out_shape=jax.ShapeDtypeStruct((inner, outer, share, local_pairs), jnp.float32),
        in_specs=[vmem] * 7,
        out_specs=vmem,
        scratch_shapes=[
            pltpu.VMEM((2, rows, NP), jnp.float32),
            pltpu.VMEM((groups, 1, own_rows * SLOTS), jnp.int32),
            pltpu.VMEM((2, NP), jnp.float32),
            pltpu.VMEM((2 * blocks * Q, 2 * NP), jnp.bfloat16),
            pltpu.VMEM((chunks, inner, outer, share, width), jnp.float32),
            pltpu.VMEM((chunks, inner, outer, share, width), jnp.float32),
            pltpu.VMEM((chunks, outer, share, width), jnp.float32),
            pltpu.VMEM((chunks, outer, share, width), jnp.float32),
            pltpu.VMEM((chunks, share, width), jnp.float32),
            dma((groups,)), dma((groups,)), dma, dma,
            dma((chunks, inner)), dma((chunks, inner)), dma((chunks, outer)), dma((chunks, outer)),
            dma((chunks, outer)), dma((chunks, outer)), dma((chunks, inner)), dma((chunks, inner)),
        ],
        compiler_params=pltpu.CompilerParams(collective_id=0, has_side_effects=True),
    )(
        signal, hop_offsets.reshape(1, own_rows * SLOTS), pair_channels,
        first_high, first_low, second_both, second_low,
    )
    return surface.reshape(Q, local_pairs)


def solution(mesh):
    return jax.shard_map(
        functools.partial(shards, mesh.shape["tm"], mesh.shape["pair"]),
        mesh=mesh,
        in_specs=(P(None, "tm"), P(("tm", "pair")), P(None, "pair")),
        out_specs=P(None, "pair"),
        check_vma=False,
    )
```
